128 devices in a mesh: cuts: 8 (over z, x_lo), row: 16 (over x_hi, y, core).
Axes of the slice: x: 4 (x_hi: 2, x_lo: 2; x = x_hi * 2 + x_lo), y: 4, z: 4, core: 2. Of those that a mesh axis runs over, the one named last changes fastest.
Arguments:
- eigvecs: float32 [16384, 4096], P('row', 'cuts'), may hold values from -1.2 to 1.2
- slice_counts: int32 [8], P('cuts'), may hold values from 256 to 512, as said below
- occ_index: int32 [4096], P('cuts'), may hold values from 0 to 63
- occ_levels: float32 [64], replicated, may hold values from 0 to 1
Outputs:
- slab: float32 [4096, 16384], P('cuts', 'row')
The draws below stay inside these ranges and needn't reach their ends.
Inputs may be any that keep to these rules, and one draw needn't show every extreme that they name: `slice_counts`: some slice holds exactly 512 eigenvalues in every draw; the others at least half of that.
All inputs are finite; a program needn't handle non-finite values.
Results may differ from the reference program's by a relative error of at most 0.000062.
Values sent between devices are 32-bit elements; how exact they have to be, the bound alone decides.
No kernel may reach another device: no remote copies, remote signals or barrier semaphores. Data moves between devices by JAX's collectives and lax.ppermute only.
A program may use at most 128 MiB of HBM per device.

```python
import jax
import jax.numpy as jnp
from jax import lax

ORDER = 16384
BLOCK = 1024
SLAB_SUB = 256
EIG_DEV = 512
LEVELS = 64
EIGS = 4096
SLAB = 4096
N_CUTS = 8


def draw_slice_counts(key, part):
    first, second = jax.random.split(jax.random.fold_in(key, 11))
    counted = jax.random.randint(first, (N_CUTS,), EIG_DEV // 2, EIG_DEV + 1)
    full_one = jax.random.randint(second, (), 0, N_CUTS)
    return jnp.where(jnp.arange(N_CUTS) == full_one, EIG_DEV, counted).astype(jnp.int32)


def with_ends(array, stream_key, low, top_value):
    longest = array.shape.index(max(array.shape))
    spots = []
    for shift in (0, 1):
        where = [jax.random.randint(jax.random.fold_in(stream_key, axis), (), 0, length) for axis, length in enumerate(array.shape)]
        where[longest] = (where[longest] + shift) % array.shape[longest]
        spots.append(tuple(where))
    return array.at[spots[0]].set(low).at[spots[1]].set(top_value)


def block_levels(key, dims, pieces, low, largest):
    factor_of, own = 1.0, jax.random.fold_in(key, 6)
    for position, shards_of in pieces:
        draws = jnp.exp(jax.random.uniform(jax.random.fold_in(own, position), (shards_of,), jnp.float32, low / len(pieces), largest / len(pieces)))
        factor_of = factor_of * jnp.repeat(draws, dims[position] // shards_of).reshape([-1 if axis == position else 1 for axis in range(len(dims))])
    return factor_of


def gaussian(own_key, shape, width, reach, pieces=(), held_as=jnp.bfloat16):
    array = jax.random.normal(own_key, shape, jnp.float32) * width
    if len(pieces) > 0:
        array = block_levels(own_key, shape, pieces, -0.22, 0.18) * array
    return jnp.clip(array, min=-reach, max=reach).astype(held_as)


def setup_inputs(seed: int = 0) -> dict:
    key_of = jax.random.split(jax.random.key(seed), 5)
    eigvecs = gaussian(key_of[0], (ORDER, EIGS), 0.18, 1.2, ((0, 16), (1, 8)), jnp.float32)
    slice_counts = draw_slice_counts(jax.random.fold_in(key_of[4], 71), 0)
    occ_index = with_ends(jax.random.randint(key_of[2], (EIGS,), 0, LEVELS), jax.random.fold_in(key_of[2], 1), 0, LEVELS - 1).astype(jnp.int32)
    occ_levels = jnp.clip(jax.random.uniform(key_of[3], (LEVELS,), jnp.float32, 0.0, 1.0), 0.0, 1.0)
    return dict(eigvecs=eigvecs, slice_counts=slice_counts, occ_index=occ_index, occ_levels=occ_levels)


def reference(eigvecs, slice_counts, occ_index, occ_levels):
    slots = jnp.arange(EIGS, dtype=jnp.int32)
    group = slots // EIG_DEV
    inside = slots - group * EIG_DEV
    live = inside < slice_counts[group]
    weights = jnp.where(live, occ_levels[occ_index], jnp.float32(0.0))
    blocks = eigvecs.reshape(ORDER // BLOCK, BLOCK, EIGS)[:, :SLAB_SUB, :]
    picked = blocks.reshape(SLAB, EIGS) * weights[None, :]
    return lax.dot_general(picked, eigvecs, (((1,), (1,)), ((), ())), precision=lax.Precision.HIGHEST, preferred_element_type=jnp.float32)
```

```python
import functools

import jax
import jax.numpy as jnp
from jax import lax
from jax.experimental import pallas as pl
from jax.experimental.pallas import tpu as pltpu
from jax.sharding import Mesh
from jax.sharding import PartitionSpec as P

SLAB_SUB = 256
AXES = ("z", "xl", "xh", "y", "c")
SIZES = (4, 2, 2, 4, 2)
CHUNKS = 4


def rank_of(z, xl, xh, y, c):
    return (((z * 2 + xl) * 2 + xh) * 4 + y) * 2 + c


def permute(array, target):
    pairs = []
    for z in range(4):
        for xl in range(2):
            for xh in range(2):
                for y in range(4):
                    for c in range(2):
                        pairs.append((rank_of(z, xl, xh, y, c), rank_of(*target(z, xl, xh, y, c))))
    return lax.ppermute(array, AXES, pairs)


def along_z(step):
    return lambda z, xl, xh, y, c: ((z + step) % 4, xl, xh, y, c)


def to_plane(flip):
    def target(z, xl, xh, y, c):
        spot = z ^ (3 * c)
        return (xh * 2 + y // 2, xl, spot // 2, (spot % 2) * 2 + ((y % 2) ^ flip), c)

    return target


def in_plane(dxh, dy):
    return lambda z, xl, xh, y, c: (z, xl, xh ^ dxh, (y - dy) % 4, c)


def other_core(z, xl, xh, y, c):
    return (z, xl, xh, y, 1 - c)


def x_partner(z, xl, xh, y, c):
    return (z, 1 - xl, xh, y, c)


def split(value):
    high = value.astype(jnp.bfloat16)
    return high, (value - high.astype(jnp.float32)).astype(jnp.bfloat16)


def prepare_kernel(table_ref, mine_ref, theirs_ref, high_ref, low_ref):
    step = pl.program_id(0)
    for source, ref in enumerate((mine_ref, theirs_ref)):
        row = pl.multiple_of(table_ref[source * 16 + step * 2] * 128, 128)
        col = pl.multiple_of(table_ref[source * 16 + step * 2 + 1] * 512, 512)
        high, low = split(ref[...])
        high_ref[pl.ds(row, 128), pl.ds(col, 512)] = high
        low_ref[pl.ds(row, 128), pl.ds(col, 512)] = low


def prepare(table, mine, theirs):
    full = pl.BlockSpec((512, 2048), lambda i, t: (0, 0))
    piece = pl.BlockSpec((128, 512), lambda i, t: (i, 0))
    shape = jax.ShapeDtypeStruct((512, 2048), jnp.bfloat16)
    return pl.pallas_call(
        prepare_kernel,
        grid_spec=pltpu.PrefetchScalarGridSpec(
            num_scalar_prefetch=1, grid=(8,), in_specs=[piece, piece], out_specs=[full, full]
        ),
        out_shape=[shape, shape],
        cost_estimate=pl.CostEstimate(flops=8_000_000, bytes_accessed=8 << 20, transcendentals=0),
        name="prepare_rows",
    )(table, mine, theirs)


def product_kernel(high_ref, low_ref, e_ref, next_ref, far_a_ref, far_b_ref, prev_ref, o_ref, eh, el):
    half = far_a_ref.shape[0]
    for spot, (row, ref) in enumerate(
        ((0, e_ref), (0, next_ref), (0, far_a_ref), (half, far_b_ref), (0, prev_ref))
    ):
        column = (0, 1, 2, 2, 3)[spot] * 512
        high, low = split(ref[...])
        eh[row : row + ref.shape[0], column : column + 512] = high
        el[row : row + ref.shape[0], column : column + 512] = low
    dims = (((1,), (1,)), ((), ()))
    dot = functools.partial(lax.dot_general, dimension_numbers=dims, preferred_element_type=jnp.float32)
    o_ref[...] = dot(high_ref[...], eh[...]) + dot(high_ref[...], el[...]) + dot(low_ref[...], eh[...])


def product(k, high, low, e, nxt, far_a, far_b, prev):
    rows = nxt.shape[0]
    whole = lambda a: pl.BlockSpec(a.shape, lambda i: (0, 0))
    return pl.pallas_call(
        product_kernel,
        grid=(1,),
        in_specs=[whole(high), whole(low), pl.BlockSpec((rows, 512), lambda i: (k, 0)),
                  whole(nxt), whole(far_a), whole(far_b), whole(prev)],
        out_specs=pl.BlockSpec((512, rows), lambda i: (0, 0)),
        out_shape=jax.ShapeDtypeStruct((512, rows), jnp.float32),
        scratch_shapes=[pltpu.VMEM((rows, 2048), jnp.bfloat16)] * 2,
        cost_estimate=pl.CostEstimate(
            flops=6 * 512 * 2048 * rows, bytes_accessed=(4 << 20) + rows * 10240, transcendentals=0
        ),
        name="partial_slab",
    )(high, low, e, nxt, far_a, far_b, prev)


def shards(eigvecs, slice_counts, occ_index, occ_levels):
    slot_count = eigvecs.shape[1]
    z, xl, xh, y, c = (lax.axis_index(a) for a in AXES)
    level_ids = jnp.arange(occ_levels.shape[0], dtype=jnp.int32)
    one_hot = (occ_index[:, None] == level_ids[None, :]).astype(jnp.float32)
    values = jnp.dot(one_hot, occ_levels, precision=lax.Precision.HIGHEST)
    live = jnp.arange(slot_count, dtype=jnp.int32) < slice_counts[0]
    weights = jnp.where(live, values, jnp.float32(0.0))
    picked = eigvecs[:SLAB_SUB] * weights[None, :]

    upper, lower = picked[:128], picked[128:]
    odd = (y % 2) == 1
    same = permute(jnp.where(odd, lower, upper), to_plane(0))
    flipped = permute(jnp.where(odd, upper, lower), to_plane(1))
    partner_first = (y % 2) == (1 - xl)
    halves = (jnp.where(partner_first, same, flipped), jnp.where(partner_first, flipped, same))

    rows = eigvecs.shape[0] // CHUNKS
    gathered = []
    for k in range(CHUNKS):
        mine = eigvecs[k * rows : (k + 1) * rows]
        prev = permute(mine, along_z(1))
        nxt = permute(mine, along_z(-1))
        far_a = permute(prev[: rows // 2], along_z(1))
        far_b = permute(nxt[rows // 2 :], along_z(-1))
        gathered.append((nxt, far_a, far_b, prev))

    offsets = [(dxh, dy) for dy in range(4) for dxh in range(2)]
    table = []
    for core in (c, 1 - c):
        for dxh, dy in offsets:
            row = (y + dy) % 4
            source_z = ((xh ^ dxh) * 2 + row // 2) ^ (3 * core)
            table += [core * 2 + row % 2, (source_z - z) % 4]
    table = jnp.stack(table).astype(jnp.int32)

    ready = []
    for piece in halves:
        got = [piece if o == (0, 0) else permute(piece, in_plane(*o)) for o in offsets]
        mine = jnp.concatenate(got, axis=0)
        theirs = permute(mine, other_core)
        ready.append(prepare(table, mine, theirs))

    out = []
    for k in range(CHUNKS):
        theirs = product(k, *ready[0], eigvecs, *gathered[k])
        received = permute(theirs, x_partner)
        out.append(product(k, *ready[1], eigvecs, *gathered[k]) + received)
    return jnp.concatenate(out, axis=1)


def solution(mesh):
    finer = Mesh(mesh.devices.reshape(SIZES), AXES)
    cuts, row = ("z", "xl"), ("xh", "y", "c")
    in_specs = (P(row, cuts), P(cuts), P(cuts), P())
    return jax.shard_map(
        shards, mesh=finer, in_specs=in_specs, out_specs=P(cuts, row), check_vma=False
    )
```
